32 devices in a mesh: src: 4 (over y, core), dst: 8 (over z, x).
Axes of the slice: x: 2, y: 2, z: 4, core: 2. Of those that a mesh axis runs over, the one named last changes fastest.
Arguments:
- normed: bfloat16 [2, 16384], replicated, may hold values from -15 to 15
- qkv_weight: bfloat16 [16384, 18432], P(('src', 'dst')), may hold values from -0.046875 to 0.046875
- out_weight: bfloat16 [16384, 16384], P('dst', 'src'), may hold values from -0.046875 to 0.046875
- prefill_pool: bfloat16 [128, 8, 64, 256], P('src', 'dst'), may hold values from -52 to 52
- page_table: int32 [2, 96], replicated, may hold values from 0 to 127, as said below
- lengths: int32 [2], replicated, may hold values from 1985 to 6144, as said below
- selected: int32 [2, 8, 32], replicated, may hold values from 0 to 95, as said below
- handoff: int32 [1, 128], replicated, may hold values from 0 to 3, as said below
Outputs:
- attn_out: float32 [2, 16384], P(None, 'src')
- decode_pool: bfloat16 [128, 8, 64, 256], P('src', 'dst')
The draws below stay inside these ranges and needn't reach their ends.
Inputs may be any that keep to these rules, and one draw needn't show every extreme that they name: `page_table`: within each group the pages of its 2 requests, ceil(lengths / 64) each, fill every slot of the group's pool exactly once; a request's pages lie in page order over owners (owner = slot // 32); entries past a request's last page are 0. `lengths`: each request has 32 or more pages; in each group the page counts sum to 128 and one request has exactly 96 pages. `selected`: distinct page numbers below the request's page count. `handoff`: each decoder index receives exactly 32 slots of every group and at most 9 of one owner's slots; in every group some owner hands exactly 9 slots to some decoder.
All inputs are finite; a program needn't handle non-finite values.
Results may differ from the reference program's by a relative error of at most 0.02.
The reference program's roundings to bfloat16 on the way count: a program that leaves them out, or rounds other values in their place, can miss the bound.
Values may be sent and summed in bfloat16 or wider, within the bound.
No kernel may reach another device: no remote copies, remote signals or barrier semaphores. Data moves between devices by JAX's collectives and lax.ppermute only.
A program may use at most 128 MiB of HBM per device.

```python
import jax
import jax.numpy as jnp
from jax import lax

D = 16384
QH = 128
KVH = 8
HD = 128
PAGE = 64
NSEL = 32
REQ_G = 2
SLOTS = 32
GROUPS = 1
REQ = 2
GRP = 16
MAXP = 96
N_SRC = 4
N_DST = 8


def layout(key):
    slot_total = N_SRC * SLOTS
    keys_all = jax.random.split(key, 9)
    spare = slot_total - MAXP - (REQ_G - 1) * NSEL
    cut_points = jnp.sort(jax.random.randint(keys_all[0], (GROUPS, REQ_G - 2), 0, spare + 1), axis=1)
    edges = jnp.concatenate([jnp.zeros((GROUPS, 1), jnp.int32), cut_points, jnp.full((GROUPS, 1), spare, jnp.int32)], axis=1)
    others = jnp.diff(edges, axis=1) + NSEL
    big_member = jax.random.randint(keys_all[1], (GROUPS, 1), 0, REQ_G)
    member_index = jnp.arange(REQ_G, dtype=jnp.int32)[None, :]
    shifted = member_index - (member_index > big_member).astype(jnp.int32)
    padded = jnp.concatenate([others, jnp.zeros((GROUPS, 1), jnp.int32)], axis=1)
    page_counts = jnp.where(member_index == big_member, MAXP, jnp.take_along_axis(padded, jnp.clip(shifted, 0, REQ_G - 1), axis=1))
    tail_tokens = jax.random.randint(keys_all[2], (GROUPS, REQ_G), 1, PAGE + 1)
    token_counts = (page_counts - 1) * PAGE + tail_tokens
    seq_order = jax.vmap(lambda sub_key: jax.random.permutation(sub_key, REQ_G))(jax.random.split(keys_all[3], GROUPS)).astype(jnp.int32)
    counts_ordered = jnp.take_along_axis(page_counts, seq_order, axis=1)
    starts_ordered = jnp.cumsum(counts_ordered, axis=1) - counts_ordered
    inverse_order = jnp.argsort(seq_order, axis=1)
    starts = jnp.take_along_axis(starts_ordered, inverse_order, axis=1)
    slot_perm = jax.vmap(lambda sub_key: jax.random.permutation(sub_key, SLOTS))(jax.random.split(keys_all[4], GROUPS * N_SRC)).astype(jnp.int32)
    slot_perm = slot_perm.reshape(GROUPS, N_SRC * SLOTS)
    page_index = jnp.arange(MAXP, dtype=jnp.int32)
    sequence_pos = starts[:, :, None] + page_index[None, None, :]
    is_valid = page_index[None, None, :] < page_counts[:, :, None]
    safe_pos = jnp.where(is_valid, sequence_pos, 0)
    owners = safe_pos // SLOTS
    within = jnp.take_along_axis(slot_perm, safe_pos.reshape(GROUPS, -1), axis=1).reshape(GROUPS, REQ_G, MAXP)
    table = jnp.where(is_valid, owners * SLOTS + within, 0).reshape(REQ, MAXP)
    sigma = jax.vmap(lambda sub_key: jax.random.permutation(sub_key, N_SRC))(jax.random.split(keys_all[5], GROUPS)).astype(jnp.int32)
    offset = jax.random.randint(keys_all[6], (GROUPS, 1), 1, N_SRC)
    decoders = jnp.arange(N_SRC, dtype=jnp.int32)[None, None, :]
    plus_one = (decoders == sigma[:, :, None]).astype(jnp.int32)
    minus_one = (decoders == ((sigma + offset) % N_SRC)[:, :, None]).astype(jnp.int32)
    sends = SLOTS // N_SRC + plus_one - minus_one
    running = jnp.cumsum(sends, axis=2)
    positions = jnp.arange(SLOTS, dtype=jnp.int32)
    decoder_of_pos = jnp.sum((running[:, :, None, :] <= positions[None, None, :, None]).astype(jnp.int32), axis=3)
    spread_perm = jax.vmap(lambda sub_key: jax.random.permutation(sub_key, SLOTS))(jax.random.split(keys_all[7], GROUPS * N_SRC)).astype(jnp.int32)
    spread_inverse = jnp.argsort(spread_perm.reshape(GROUPS, N_SRC, SLOTS), axis=2)
    handoff_table = jnp.take_along_axis(decoder_of_pos, spread_inverse, axis=2).reshape(GROUPS, N_SRC * SLOTS)
    flat_counts = page_counts.reshape(REQ)
    raw_scores = jax.random.randint(keys_all[8], (REQ, KVH, MAXP), 0, 2 ** 18) * MAXP + page_index[None, None, :]
    raw_scores = jnp.where(page_index[None, None, :] < flat_counts[:, None, None], raw_scores, -1)
    picked_scores, picked = lax.top_k(raw_scores, NSEL)
    return (table.astype(jnp.int32), token_counts.reshape(REQ).astype(jnp.int32), picked.astype(jnp.int32), handoff_table.astype(jnp.int32))


def draw_page_table(key, part):
    return layout(jax.random.fold_in(key, 5))[0]


def draw_lengths(key, part):
    return layout(jax.random.fold_in(key, 5))[1]


def draw_selected(key, part):
    return layout(jax.random.fold_in(key, 5))[2]


def draw_handoff(key, part):
    return layout(jax.random.fold_in(key, 5))[3]


def draw_prefill_pool(key, part):
    key_first, key_second = jax.random.split(jax.random.fold_in(key, 11), 2)
    shape = (N_SRC * SLOTS, N_DST, PAGE, HD)
    key_part = jnp.clip(jax.random.normal(key_first, shape), -6.0, 6.0)
    value_part = jnp.clip(jax.random.normal(key_second, shape), -6.0, 6.0)
    return jnp.concatenate([key_part, value_part], axis=-1).astype(jnp.bfloat16)


def steps_of(own_key, dims, cuts, low, high):
    gain, own = 1.0, jax.random.fold_in(own_key, 6)
    for dim, shards_of in cuts:
        steps = jnp.exp(jax.random.uniform(jax.random.fold_in(own, dim), (shards_of,), jnp.float32, low / len(cuts), high / len(cuts)))
        gain = gain * jnp.repeat(steps, dims[dim] // shards_of).reshape([-1 if axis == dim else 1 for axis in range(len(dims))])
    return gain


def centred(rng, shape, scale, bound, pieces=(), kind=jnp.bfloat16):
    values = jax.random.normal(rng, shape, jnp.float32) * scale
    if len(pieces) > 0:
        values = steps_of(rng, shape, pieces, -0.22, 0.18) * values
    return jnp.clip(values, min=-bound, max=bound).astype(kind)


def setup_inputs(seed: int = 0) -> dict:
    streams_of = jax.random.split(jax.random.key(seed), 9)
    normed = centred(streams_of[0], (REQ, D), 2.5, 15.0)
    qkv_weight = centred(streams_of[1], (D, KVH * (GRP + 2) * HD), D ** -0.5, 0.046875, ((0, 32),))
    out_weight = centred(streams_of[2], (QH * HD, D), (QH * HD) ** -0.5, 0.046875, ((0, 8), (1, 4)))
    prefill_pool = draw_prefill_pool(jax.random.fold_in(streams_of[8], 71), 0)
    page_table = draw_page_table(jax.random.fold_in(streams_of[8], 71), 0)
    lengths = draw_lengths(jax.random.fold_in(streams_of[8], 71), 0)
    selected = draw_selected(jax.random.fold_in(streams_of[8], 71), 0)
    handoff = draw_handoff(jax.random.fold_in(streams_of[8], 71), 0)
    return dict(normed=normed, qkv_weight=qkv_weight, out_weight=out_weight, prefill_pool=prefill_pool, page_table=page_table, lengths=lengths, selected=selected, handoff=handoff)


NEG_FILL = -1.0e30
ROPE_BASE = 500000.0


def rotate(vectors, positions):
    half_dim = vectors.shape[-1] // 2
    frequency = ROPE_BASE ** (-2.0 * jnp.arange(half_dim, dtype=jnp.float32) / vectors.shape[-1])
    angles = positions[..., None] * frequency
    cosine = jnp.cos(angles)
    sine_part = jnp.sin(angles)
    first_half = vectors[..., :half_dim]
    second = vectors[..., half_dim:]
    return jnp.concatenate([first_half * cosine - second * sine_part, second * cosine + first_half * sine_part], axis=-1)


def reference(normed, qkv_weight, out_weight, prefill_pool, page_table, lengths, selected, handoff):
    groups = N_DST // KVH
    req_group = REQ // groups
    heads_q = QH // KVH
    slot_total = N_SRC * SLOTS
    projected = jnp.dot(normed, qkv_weight, preferred_element_type=jnp.float32).reshape(REQ, KVH, heads_q + 2, HD)
    positions = lengths.astype(jnp.float32)
    queries = (rotate(projected[:, :, :heads_q], positions[:, None, None]) * HD ** -0.5).astype(jnp.bfloat16)
    key_new = rotate(projected[:, :, heads_q], positions[:, None])
    value_new = projected[:, :, heads_q + 1]
    group_of = jnp.arange(REQ, dtype=jnp.int32) // req_group
    column_of = group_of[:, None] * KVH + jnp.arange(KVH, dtype=jnp.int32)[None, :]
    table_wide = jnp.broadcast_to(page_table[:, None, :], (REQ, KVH, page_table.shape[1]))
    slot_of = jnp.take_along_axis(table_wide, selected, axis=2)
    gathered = prefill_pool[slot_of, column_of[:, :, None]]
    keys_all = gathered[..., :HD].astype(jnp.float32)
    values_all = gathered[..., HD:].astype(jnp.float32)
    query_wide = queries.astype(jnp.float32)
    scores = jnp.einsum("rhcd,rhnpd->rhcnp", query_wide, keys_all)
    token_pos = selected[..., None] * PAGE + jnp.arange(PAGE, dtype=jnp.int32)
    key_mask = (token_pos < lengths[:, None, None, None])[:, :, None]
    own_score = jnp.sum(query_wide * key_new[:, :, None, :], axis=-1)
    top_score = jnp.maximum(jnp.max(jnp.where(key_mask, scores, NEG_FILL), axis=(3, 4)), own_score)
    weight = jnp.where(key_mask, jnp.exp(scores - top_score[..., None, None]), 0.0)
    own_weight = jnp.exp(own_score - top_score)
    weighted = jnp.einsum("rhcnp,rhnpd->rhcd", weight.astype(jnp.bfloat16).astype(jnp.float32), values_all)
    numerator = weighted + own_weight[..., None] * value_new[:, :, None, :]
    denominator = jnp.sum(weight, axis=(3, 4)) + own_weight
    attended = (numerator / denominator[..., None]).astype(jnp.bfloat16)
    attn_out = jnp.dot(attended.reshape(REQ, QH * HD), out_weight, preferred_element_type=jnp.float32)
    sort_keys = handoff * slot_total + jnp.arange(slot_total, dtype=jnp.int32)[None, :]
    slot_order = jnp.argsort(sort_keys, axis=1)
    pool_split = prefill_pool.reshape(slot_total, groups, KVH, PAGE, 2 * HD)
    moved = pool_split[jnp.transpose(slot_order)[:, :, None], jnp.arange(groups)[None, :, None], jnp.arange(KVH)[None, None, :]]
    decode_pool = moved.reshape(slot_total, N_DST, PAGE, 2 * HD)
    return attn_out, decode_pool
```

```python
import functools

import jax
import jax.numpy as jnp
import numpy as np
from jax import lax
from jax.experimental import pallas as pl
from jax.experimental.pallas import tpu as pltpu
from jax.sharding import PartitionSpec as P

QH = 128
KVH = 8
GRP = QH // KVH

NEG_FILL = -1e30
ROPE_BASE = 500000.0

SMEM = pl.BlockSpec(memory_space=pltpu.SMEM)
VMEM = pl.BlockSpec(memory_space=pltpu.VMEM)
ANY = pl.BlockSpec(memory_space=pl.ANY)


def frequencies(head_dim):
    half = np.arange(head_dim // 2, dtype=np.float64)
    frequency = ROPE_BASE ** (-2.0 * half / head_dim)
    return np.concatenate([frequency, frequency]).astype(np.float32)


def pack_body(handoff, pool, packed, count, sem):
    owners = packed.shape[0]
    slots = pool.shape[0]
    group = lax.axis_index("dst") // KVH
    first = lax.axis_index("src") * slots
    for decoder in range(owners):
        count[decoder] = 0

    def send(slot, carry):
        decoder = handoff[group, first + slot]
        place = count[decoder]
        count[decoder] = place + 1
        pltpu.make_async_copy(pool.at[slot], packed.at[decoder, place], sem).start()
        return carry

    lax.fori_loop(0, slots, send, 0)
    pltpu.make_async_copy(pool, pool, sem).wait()


def pack(handoff, pool, owners, capacity):
    return pl.pallas_call(
        pack_body,
        out_shape=jax.ShapeDtypeStruct((owners, capacity) + pool.shape[1:], pool.dtype),
        in_specs=[SMEM, ANY],
        out_specs=ANY,
        scratch_shapes=[pltpu.SMEM((owners,), jnp.int32), pltpu.SemaphoreType.DMA],
        name="pack",
    )(handoff, pool)


def project_body(
    page_len, handoff, table, lengths, selected, frequency, tokens, weight,
    out, live, cosine, sine, source, limit,
):
    groups, _, rows, head_dim = out.shape
    parts = GRP + 2
    reqs = rows // parts
    slots = source.shape[0] // 2
    step = pl.program_id(0)
    me = lax.axis_index("src")
    group = lax.axis_index("dst") // KVH
    head = lax.axis_index("dst") % KVH

    result = jnp.dot(tokens[...], weight[...], preferred_element_type=jnp.float32)
    for g in range(groups):
        for part in range(parts):
            out[g, 0, part * reqs : (part + 1) * reqs, :] = result[
                g * reqs : (g + 1) * reqs, part * head_dim : (part + 1) * head_dim
            ]

    @pl.when(step == 1)
    def _():
        def clear(index, carry):
            limit[index] = 0
            return carry

        lax.fori_loop(0, reqs * slots, clear, 0)
        for r in range(reqs):
            length = lengths[group * reqs + r]

            def mark(entry, carry, r=r, length=length):
                page = selected[group * reqs + r, head, entry]
                slot = table[group * reqs + r, page]
                mine = slot // slots == me
                place = jnp.where(mine, r * slots + slot % slots, reqs * slots)
                limit[place] = length - page * page_len
                return carry

            lax.fori_loop(0, selected.shape[2], mark, 0)

    @pl.when(step == 2)
    def _():
        lane = lax.broadcasted_iota(jnp.int32, (1, 128), 1)
        per = 128 // page_len
        for r in range(reqs):
            for chunk in range(slots // per):
                bound = jnp.full((1, 128), limit[r * slots + chunk * per], jnp.int32)
                for k in range(1, per):
                    bound = jnp.where(
                        lane >= k * page_len, limit[r * slots + chunk * per + k], bound
                    )
                live[r : r + 1, chunk * 128 : (chunk + 1) * 128] = jnp.where(
                    lane % page_len < bound, 1.0, 0.0
                )

    @pl.when(step == 3)
    def _():
        lane = lax.broadcasted_iota(jnp.int32, (1, head_dim), 1)
        for r in range(reqs):
            position = lengths[group * reqs + r].astype(jnp.float32)
            angle = frequency[...] * position
            cosine[r : r + 1, :] = jnp.cos(angle)
            sine[r : r + 1, :] = jnp.where(lane < head_dim // 2, -jnp.sin(angle), jnp.sin(angle))

    @pl.when(step == 4)
    def _():
        owners = handoff.shape[1] // slots
        capacity = slots // owners + 1

        def owner_pages(owner, filled):
            def look(slot, state):
                filled, taken = state
                hit = handoff[group, owner * slots + slot] == me
                source[jnp.where(hit, filled, slots)] = owner * capacity + taken
                one = hit.astype(jnp.int32)
                return filled + one, taken + one

            return lax.fori_loop(0, slots, look, (filled, 0))[0]

        lax.fori_loop(0, owners, owner_pages, 0)


def project(handoff, table, lengths, selected, tokens, weight, groups, slots, page_len):
    reqs_all, rows = tokens.shape
    reqs = reqs_all // groups
    width = weight.shape[1] // KVH
    head_dim = width // (GRP + 2)
    frequency = jnp.asarray(frequencies(head_dim))[None]

    def fixed(shape):
        return pl.BlockSpec(shape, lambda i: (0,) * len(shape))

    return pl.pallas_call(
        functools.partial(project_body, page_len),
        grid=(KVH,),
        in_specs=[
            SMEM, SMEM, SMEM, SMEM,
            fixed((1, head_dim)),
            fixed((reqs_all, rows)),
            pl.BlockSpec((rows, width), lambda i: (0, i)),
        ],
        out_specs=[
            pl.BlockSpec((groups, 1, (GRP + 2) * reqs, head_dim), lambda i: (0, i, 0, 0)),
            fixed((reqs, slots * page_len)),
            fixed((reqs, head_dim)),
            fixed((reqs, head_dim)),
            SMEM,
        ],
        out_shape=[
            jax.ShapeDtypeStruct((groups, KVH, (GRP + 2) * reqs, head_dim), jnp.float32),
            jax.ShapeDtypeStruct((reqs, slots * page_len), jnp.float32),
            jax.ShapeDtypeStruct((reqs, head_dim), jnp.float32),
            jax.ShapeDtypeStruct((reqs, head_dim), jnp.float32),
            jax.ShapeDtypeStruct((2 * slots,), jnp.int32),
        ],
        scratch_shapes=[pltpu.SMEM((reqs * slots + 1,), jnp.int32)],
        compiler_params=pltpu.CompilerParams(vmem_limit_bytes=24 * 1024 * 1024),
        name="project",
    )(handoff, table, lengths, selected, frequency, tokens, weight)


def attend_body(parts, pool, live, cosine, sine, out):
    total = parts[0]
    for source in range(1, parts.shape[0]):
        total = total + parts[source]
    head_dim = total.shape[1]
    reqs = live.shape[0]
    rows = GRP * reqs

    def per_row(values, count):
        row = lax.broadcasted_iota(jnp.int32, (count, 1), 0) % reqs
        wide = jnp.broadcast_to(values[0:1], (count, values.shape[1]))
        for r in range(1, reqs):
            wide = jnp.where(row == r, values[r : r + 1], wide)
        return wide

    turned = total[: rows + reqs]
    turned = turned * per_row(cosine[...], rows + reqs) + pltpu.roll(
        turned, head_dim // 2, 1
    ) * per_row(sine[...], rows + reqs)
    queries = (turned[:rows] * head_dim ** (-0.5)).astype(jnp.bfloat16)
    key_new = per_row(turned[rows:], rows)
    value_new = per_row(total[rows + reqs :], rows)

    pages = pool[...].reshape(-1, 2 * head_dim)
    scores = lax.dot_general(
        queries, pages[:, :head_dim], (((1,), (1,)), ((), ())),
        preferred_element_type=jnp.float32,
    )
    mask = per_row(live[...], rows) > 0.5
    own = jnp.sum(queries.astype(jnp.float32) * key_new, axis=1, keepdims=True)
    first = lax.axis_index("src") == 0
    own = jnp.where(first, own, NEG_FILL)
    top = jnp.maximum(jnp.max(jnp.where(mask, scores, NEG_FILL), axis=1, keepdims=True), own)
    weight = jnp.where(mask, jnp.exp(scores - top), 0.0)
    own_weight = jnp.where(first, jnp.exp(own - top), 0.0)
    total_weight = jnp.sum(weight, axis=1, keepdims=True) + own_weight
    weighted = (
        jnp.dot(
            weight.astype(jnp.bfloat16), pages[:, head_dim:], preferred_element_type=jnp.float32
        )
        + own_weight * value_new
    )
    out[:, :head_dim] = weighted
    lane = lax.broadcasted_iota(jnp.int32, (rows, head_dim), 1)
    out[:, head_dim:] = jnp.where(lane < head_dim // 2, top, total_weight)


def attend(parts, pool, live, cosine, sine):
    reqs = live.shape[0]
    return pl.pallas_call(
        attend_body,
        out_shape=jax.ShapeDtypeStruct((GRP * reqs, pool.shape[2]), jnp.float32),
        in_specs=[VMEM] * 5,
        out_specs=VMEM,
        compiler_params=pltpu.CompilerParams(vmem_limit_bytes=16 * 1024 * 1024),
        name="attend",
    )(parts, pool, live, cosine, sine)


def merge(parts):
    head_dim = parts.shape[-1] // 2
    half = head_dim + head_dim // 2
    tops = [parts[s, :, head_dim : head_dim + 1] for s in range(parts.shape[0])]
    overall = functools.reduce(jnp.maximum, tops)
    numerator = denominator = 0.0
    for s, top in enumerate(tops):
        factor = jnp.exp(top - overall)
        numerator = numerator + parts[s, :, :head_dim] * factor
        denominator = denominator + parts[s, :, half : half + 1] * factor
    return numerator / denominator


def output_body(merged, source, heads, pages, weight, out, pool, tokens, sem):
    step = pl.program_id(0)
    slots = pool.shape[0]
    copies = out.shape[0]
    depth = weight.shape[0]

    @pl.when(step == 0)
    def _():
        def place(slot, carry):
            pltpu.make_async_copy(pages.at[source[slot]], pool.at[slot], sem).start()
            return carry

        lax.fori_loop(0, slots, place, 0)
        if merged:
            reqs = tokens.shape[0]
            attended = merge(heads)
            head_dim = attended.shape[1]
            for c in range(GRP):
                tokens[:, c * head_dim : (c + 1) * head_dim] = attended[c * reqs : (c + 1) * reqs]
        else:
            tokens[...] = heads[...].astype(jnp.float32)

    result = jnp.dot(
        tokens[...].astype(jnp.bfloat16), weight[...], preferred_element_type=jnp.float32
    ).astype(out.dtype)
    for copy in range(copies):
        out[copy] = result

    @pl.when(step == pl.num_programs(0) - 1)
    def _():
        pltpu.make_async_copy(pool, pool, sem).wait()


def output(source, heads, pages, weight, reqs, copies, slots, merged):
    depth, width = weight.shape
    tile = width // 8 if width % 1024 == 0 else width
    return pl.pallas_call(
        functools.partial(output_body, merged),
        grid=(width // tile,),
        in_specs=[
            SMEM,
            pl.BlockSpec(heads.shape, lambda i: (0,) * heads.ndim),
            ANY,
            pl.BlockSpec((depth, tile), lambda i: (0, i)),
        ],
        out_specs=[pl.BlockSpec((copies, reqs, tile), lambda i: (0, 0, i)), ANY],
        out_shape=[
            jax.ShapeDtypeStruct((copies, reqs, width), jnp.bfloat16),
            jax.ShapeDtypeStruct((slots,) + pages.shape[1:], pages.dtype),
        ],
        scratch_shapes=[pltpu.VMEM((reqs, depth), jnp.float32), pltpu.SemaphoreType.DMA],
        compiler_params=pltpu.CompilerParams(vmem_limit_bytes=24 * 1024 * 1024),
        name="output",
    )(source, heads, pages, weight)


def shards(normed, qkv_weight, out_weight, prefill_pool, page_table, lengths, selected, handoff):
    owners = lax.axis_size("src")
    decoders = lax.axis_size("dst")
    decoder_id = lax.axis_index("dst")
    groups = decoders // KVH
    reqs = normed.shape[0]
    req_group = reqs // groups
    pool = prefill_pool.reshape(prefill_pool.shape[0], *prefill_pool.shape[2:])
    slots, page_len = pool.shape[:2]
    capacity = slots // owners + 1

    packed = pack(handoff, pool, owners, capacity)
    arrived = lax.all_to_all(packed, "src", split_axis=0, concat_axis=0, tiled=True)

    rows = qkv_weight.shape[0]
    row_block = lax.axis_index("src") * decoders + decoder_id
    tokens = lax.dynamic_slice_in_dim(normed, row_block * rows, rows, 1)
    partial, live, cosine, sine, source = project(
        handoff, page_table, lengths, selected, tokens, qkv_weight, groups, slots, page_len
    )
    shares = lax.all_to_all(
        partial.reshape((decoders,) + partial.shape[2:]), "dst",
        split_axis=0, concat_axis=0, tiled=True,
    )
    projected = lax.all_gather(jnp.sum(shares, axis=0), "src")
    mine = attend(projected, pool, live, cosine, sine)
    heads = lax.all_gather(mine, "src")
    merged = groups == 1
    if not merged:
        attended = merge(heads).astype(jnp.bfloat16)
        head_dim = attended.shape[1]
        flat = attended.reshape(GRP, req_group, head_dim).transpose(1, 0, 2)
        every = lax.all_gather(flat.reshape(req_group, -1), "dst", axis=0, tiled=True)
        every = every.reshape(groups, KVH, req_group, -1)
        block = lax.dynamic_index_in_dim(every, decoder_id // groups, 1, keepdims=False)
        depth = out_weight.shape[0]
        heads = lax.dynamic_slice_in_dim(
            block.reshape(reqs, -1), (decoder_id % groups) * depth, depth, 1
        )
    outgoing, decode_pool = output(
        source, heads, arrived.reshape((-1,) + pool.shape[1:]), out_weight,
        reqs, decoders, slots, merged,
    )
    incoming = lax.all_to_all(outgoing, "dst", split_axis=0, concat_axis=0, tiled=True)
    attn_out = jnp.sum(incoming.astype(jnp.float32), axis=0)
    return attn_out, decode_pool[:, None]


def solution(mesh):
    return jax.shard_map(
        shards,
        mesh=mesh,
        in_specs=(
            P(),
            P(("src", "dst"), None),
            P("dst", "src"),
            P("src", "dst", None, None),
            P(),
            P(),
            P(),
            P(),
        ),
        out_specs=(P(None, "src"), P("src", "dst", None, None)),
        check_vma=False,
    )
```

```python
import functools

import jax
import jax.numpy as jnp
import numpy as np
from jax import lax
from jax.experimental import pallas as pl
from jax.experimental.pallas import tpu as pltpu
from jax.sharding import PartitionSpec as P


QH = 128
KVH = 8
GRP = QH // KVH


NEG_FILL = -1e30
ROPE_BASE = 500000.0

SMEM = pl.BlockSpec(memory_space=pltpu.SMEM)
VMEM = pl.BlockSpec(memory_space=pltpu.VMEM)
ANY = pl.BlockSpec(memory_space=pl.ANY)


def near(array):
    return pltpu.with_memory_space_constraint(array, pltpu.HBM)


def frequencies(head_dim):
    half = np.arange(head_dim // 2, dtype=np.float64)
    frequency = ROPE_BASE ** (-2.0 * half / head_dim)
    return np.concatenate([frequency, frequency]).astype(np.float32)


def pack_body(handoff, pool, *rest):
    packed, (count, sem) = rest[:-2], rest[-2:]
    owners = len(packed) + 1
    slots = pool.shape[0]
    group = lax.axis_index("dst") // KVH
    me = lax.axis_index("src")
    for offset in range(owners):
        count[offset] = 0

    def send(slot, carry):
        offset = handoff[group, me * slots + slot] ^ me
        place = count[offset]
        count[offset] = place + 1
        for other in range(1, owners):

            @pl.when(offset == other)
            def _(other=other):
                pltpu.make_async_copy(pool.at[slot], packed[other - 1].at[place], sem).start()

        return carry

    lax.fori_loop(0, slots, send, 0)

    def settle(index, carry):
        pltpu.make_async_copy(pool.at[0], packed[0].at[0], sem).wait()
        return carry

    lax.fori_loop(0, slots - count[0], settle, 0)


def pack(handoff, pool, owners, capacity):
    one = pltpu.VMEM((capacity,) + pool.shape[1:], pool.dtype)
    return pl.pallas_call(
        pack_body,
        out_shape=[one] * (owners - 1),
        in_specs=[SMEM, ANY],
        out_specs=[VMEM] * (owners - 1),
        scratch_shapes=[pltpu.SMEM((owners,), jnp.int32), pltpu.SemaphoreType.DMA],
        compiler_params=pltpu.CompilerParams(vmem_limit_bytes=4 * 1024 * 1024),
        cost_estimate=pl.CostEstimate(flops=10**10, bytes_accessed=2**25, transcendentals=0),
        name="pack",
    )(near(handoff), near(pool))


def project_body(tokens, weight, _after, out):
    groups, heads, rows, head_dim = out.shape
    parts = GRP + 2
    reqs = rows // parts
    depth = weight.shape[0]
    if tokens.shape[1] != depth:
        block = lax.axis_index("src") * lax.axis_size("dst") + lax.axis_index("dst")
        values = tokens[:, pl.ds(pl.multiple_of(block * depth, depth), depth)]
    else:
        values = tokens[...]
    width = parts * head_dim
    for head in range(heads):
        result = jnp.dot(
            values, weight[:, head * width : (head + 1) * width],
            preferred_element_type=jnp.float32,
        )
        for g in range(groups):
            for part in range(parts):
                out[g, head, part * reqs : (part + 1) * reqs, :] = result[
                    g * reqs : (g + 1) * reqs, part * head_dim : (part + 1) * head_dim
                ]


def project(tokens, weight, groups, after):
    reqs = tokens.shape[0] // groups
    parts = GRP + 2
    head_dim = weight.shape[1] // (KVH * parts)
    return pl.pallas_call(
        project_body,
        in_specs=[VMEM, VMEM, ANY],
        out_specs=VMEM,
        out_shape=pltpu.VMEM((groups, KVH, parts * reqs, head_dim), jnp.float32),
        compiler_params=pltpu.CompilerParams(vmem_limit_bytes=24 * 1024 * 1024),
        name="project",
    )(tokens, weight, after)


def plan_body(
    page_len, slots, handoff, table, lengths, selected, frequency, live, cosine, sine, source, limit
):
    reqs, head_dim = cosine.shape
    me = lax.axis_index("src")
    group = lax.axis_index("dst") // KVH
    head = lax.axis_index("dst") % KVH

    def clear(index, carry):
        limit[index] = 0
        return carry

    lax.fori_loop(0, reqs * slots, clear, 0, unroll=16)
    for r in range(reqs):
        length = lengths[group * reqs + r]

        def mark(entry, carry, r=r, length=length):
            page = selected[group * reqs + r, head, entry]
            slot = table[group * reqs + r, page]
            local = slot - me * slots
            mine = (local >= 0) & (local < slots)
            place = jnp.where(mine, r * slots + local, reqs * slots)
            limit[place] = length - page * page_len
            return carry

        lax.fori_loop(0, selected.shape[2], mark, 0, unroll=8)

    lane = lax.broadcasted_iota(jnp.int32, (1, 128), 1)
    per = 128 // page_len
    for r in range(reqs):
        for chunk in range(slots // per):
            bound = jnp.full((1, 128), limit[r * slots + chunk * per], jnp.int32)
            for k in range(1, per):
                bound = jnp.where(lane >= k * page_len, limit[r * slots + chunk * per + k], bound)
            live[r : r + 1, chunk * 128 : (chunk + 1) * 128] = jnp.where(
                lane % page_len < bound, 1.0, 0.0
            )

    row = lax.broadcasted_iota(jnp.int32, (reqs, head_dim), 0)
    place = lax.broadcasted_iota(jnp.int32, (reqs, head_dim), 1)
    position = jnp.zeros((reqs, head_dim), jnp.float32)
    for r in range(reqs):
        position = jnp.where(row == r, lengths[group * reqs + r].astype(jnp.float32), position)
    angle = frequency[...] * position
    cosine[...] = jnp.cos(angle)
    turn = jnp.sin(angle)
    sine[...] = jnp.where(place < head_dim // 2, -turn, turn)

    owners = handoff.shape[1] // slots

    def owner_pages(owner, filled):
        own = owner == me
        source[owners + (owner ^ me)] = filled

        def look(slot, taken):
            hit = handoff[group, owner * slots + slot] == me
            source[2 * owners + jnp.where(hit & own, taken, slots)] = slot
            return taken + hit.astype(jnp.int32)

        taken = lax.fori_loop(0, slots, look, 0, unroll=8)
        source[owner ^ me] = taken
        return filled + taken

    lax.fori_loop(0, owners, owner_pages, 0)


def plan(handoff, table, lengths, selected, head_dim, reqs, slots, page_len):
    owners = handoff.shape[1] // slots
    frequency = jnp.asarray(frequencies(head_dim))[None]
    return pl.pallas_call(
        functools.partial(plan_body, page_len, slots),
        in_specs=[SMEM] * 4 + [VMEM],
        out_specs=[VMEM] * 3 + [SMEM],
        out_shape=[
            jax.ShapeDtypeStruct((reqs, slots * page_len), jnp.float32),
            jax.ShapeDtypeStruct((reqs, head_dim), jnp.float32),
            jax.ShapeDtypeStruct((reqs, head_dim), jnp.float32),
            jax.ShapeDtypeStruct((2 * owners + slots + 1,), jnp.int32),
        ],
        scratch_shapes=[pltpu.SMEM((reqs * slots + 1,), jnp.int32)],
        compiler_params=pltpu.CompilerParams(vmem_limit_bytes=2 * 1024 * 1024),
        name="plan",
    )(near(handoff), near(table), near(lengths), near(selected), near(frequency))


def attend_body(parts, pool, live, cosine, sine, out):
    total = parts[0]
    for source in range(1, parts.shape[0]):
        total = total + parts[source]
    head_dim = total.shape[1]
    reqs = live.shape[0]
    rows = GRP * reqs

    def per_row(values, count):
        row = lax.broadcasted_iota(jnp.int32, (count, 1), 0) % reqs
        wide = jnp.broadcast_to(values[0:1], (count, values.shape[1]))
        for r in range(1, reqs):
            wide = jnp.where(row == r, values[r : r + 1], wide)
        return wide

    turned = total[: rows + reqs]
    turned = turned * per_row(cosine[...], rows + reqs) + pltpu.roll(
        turned, head_dim // 2, 1
    ) * per_row(sine[...], rows + reqs)
    queries = (turned[:rows] * head_dim ** (-0.5)).astype(jnp.bfloat16)
    key_new = per_row(turned[rows:], rows)
    value_new = per_row(total[rows + reqs :], rows)

    pages = pool[...].reshape(-1, 2 * head_dim)
    scores = lax.dot_general(
        queries, pages[:, :head_dim], (((1,), (1,)), ((), ())),
        preferred_element_type=jnp.float32,
    )
    mask = per_row(live[...], rows) > 0.5
    own = jnp.sum(queries.astype(jnp.float32) * key_new, axis=1, keepdims=True)
    first = lax.axis_index("src") == 0
    own = jnp.where(first, own, NEG_FILL)
    top = jnp.maximum(jnp.max(jnp.where(mask, scores, NEG_FILL), axis=1, keepdims=True), own)
    weight = jnp.where(mask, jnp.exp(scores - top), 0.0)
    own_weight = jnp.where(first, jnp.exp(own - top), 0.0)
    total_weight = jnp.sum(weight, axis=1, keepdims=True) + own_weight
    weighted = (
        jnp.dot(
            weight.astype(jnp.bfloat16), pages[:, head_dim:], preferred_element_type=jnp.float32
        )
        + own_weight * value_new
    )
    out[:, :head_dim] = weighted
    lane = lax.broadcasted_iota(jnp.int32, (rows, head_dim), 1)
    out[:, head_dim:] = jnp.where(lane < head_dim // 2, top, total_weight)


def attend(parts, pool, live, cosine, sine):
    reqs = live.shape[0]
    return pl.pallas_call(
        attend_body,
        out_shape=jax.ShapeDtypeStruct((GRP * reqs, pool.shape[2]), jnp.float32),
        in_specs=[VMEM] * 5,
        out_specs=VMEM,
        compiler_params=pltpu.CompilerParams(vmem_limit_bytes=16 * 1024 * 1024),
        cost_estimate=pl.CostEstimate(flops=10**12, bytes_accessed=2**26, transcendentals=0),
        name="attend",
    )(parts, pool, live, cosine, sine)


def merge(parts):
    head_dim = parts.shape[-1] // 2
    half = head_dim + head_dim // 2
    tops = [parts[s, :, head_dim : head_dim + 1] for s in range(parts.shape[0])]
    overall = functools.reduce(jnp.maximum, tops)
    numerator = denominator = 0.0
    for s, top in enumerate(tops):
        factor = jnp.exp(top - overall)
        numerator = numerator + parts[s, :, :head_dim] * factor
        denominator = denominator + parts[s, :, half : half + 1] * factor
    return numerator / denominator


def output_body(merged, source, heads, weight, kept, *rest):
    pages, (out, pool, tokens, stage, sem) = rest[:-5], rest[-5:]
    copies = out.shape[0]
    owners = len(pages) + 1

    def keep(index, carry):
        slot = source[2 * owners + index]
        pltpu.make_async_copy(kept.at[slot], stage.at[source[owners] + index], sem).start()
        return carry

    lax.fori_loop(0, source[0], keep, 0)
    for other in range(1, owners):

        def place(index, carry, other=other):
            target = stage.at[source[owners + other] + index]
            pltpu.make_async_copy(pages[other - 1].at[index], target, sem).start()
            return carry

        lax.fori_loop(0, source[other], place, 0)

    if merged:
        reqs = tokens.shape[0]
        attended = merge(heads)
        head_dim = attended.shape[1]
        for c in range(GRP):
            tokens[:, c * head_dim : (c + 1) * head_dim] = attended[c * reqs : (c + 1) * reqs]
        values = tokens[...].astype(jnp.bfloat16)
    else:
        values = heads[...]

    width = weight.shape[1]
    tile = width // 8 if width % 1024 == 0 else width
    ordered = pltpu.make_async_copy(stage, pool, sem)
    for start in range(0, width, tile):
        if start == width // tile // 2 * tile:
            pltpu.make_async_copy(kept, stage, sem).wait()
            ordered.start()
        result = jnp.dot(
            values, weight[:, start : start + tile], preferred_element_type=jnp.float32
        ).astype(out.dtype)
        for copy in range(copies):
            out[copy, :, start : start + tile] = result

    ordered.wait()


def output(source, heads, weight, kept, pages, reqs, copies, merged):
    depth, width = weight.shape
    return pl.pallas_call(
        functools.partial(output_body, merged),
        in_specs=[SMEM, VMEM, VMEM, ANY] + [ANY] * len(pages),
        out_specs=[VMEM, ANY],
        out_shape=[
            jax.ShapeDtypeStruct((copies, reqs, width), jnp.bfloat16),
            jax.ShapeDtypeStruct(kept.shape, kept.dtype),
        ],
        scratch_shapes=[
            pltpu.VMEM((reqs, depth), jnp.float32),
            pltpu.VMEM(kept.shape, kept.dtype),
            pltpu.SemaphoreType.DMA,
        ],
        compiler_params=pltpu.CompilerParams(vmem_limit_bytes=24 * 1024 * 1024),
        name="output",
    )(source, heads, weight, kept, *pages)


def shards(normed, qkv_weight, out_weight, prefill_pool, page_table, lengths, selected, handoff):
    owners = lax.axis_size("src")
    decoders = lax.axis_size("dst")
    decoder_id = lax.axis_index("dst")
    groups = decoders // KVH
    reqs = normed.shape[0]
    req_group = reqs // groups
    pool = prefill_pool.reshape(prefill_pool.shape[0], *prefill_pool.shape[2:])
    slots, page_len = pool.shape[:2]
    capacity = slots // owners + 1

    packed = pack(handoff, pool, owners, capacity)
    arrived = []
    for k, pages in enumerate(packed):
        arrived.append(lax.ppermute(pages, "src", [(i, i ^ (k + 1)) for i in range(owners)]))

    rows = qkv_weight.shape[0]
    tokens = normed
    if rows % 128:
        row_block = lax.axis_index("src") * decoders + decoder_id
        tokens = lax.dynamic_slice_in_dim(normed, row_block * rows, rows, 1)
    partial = project(tokens, qkv_weight, groups, packed[0])
    live, cosine, sine, source = plan(
        handoff, page_table, lengths, selected, pool.shape[2] // 2, req_group, slots, page_len
    )
    shares = lax.all_to_all(
        partial.reshape((decoders,) + partial.shape[2:]), "dst",
        split_axis=0, concat_axis=0, tiled=True,
    )
    projected = lax.all_gather(jnp.sum(shares, axis=0), "src")
    mine = attend(projected, pool, live, cosine, sine)
    heads = lax.all_gather(mine, "src")
    merged = groups == 1
    if not merged:
        attended = merge(heads).astype(jnp.bfloat16)
        head_dim = attended.shape[1]
        flat = attended.reshape(GRP, req_group, head_dim).transpose(1, 0, 2)
        every = lax.all_gather(flat.reshape(req_group, -1), "dst", axis=0, tiled=True)
        every = every.reshape(groups, KVH, req_group, -1)
        block = lax.dynamic_index_in_dim(every, decoder_id // groups, 1, keepdims=False)
        depth = out_weight.shape[0]
        heads = lax.dynamic_slice_in_dim(
            block.reshape(reqs, -1), (decoder_id % groups) * depth, depth, 1
        )
    outgoing, decode_pool = output(
        source, heads, out_weight, pool, arrived, reqs, decoders, merged
    )
    incoming = lax.all_to_all(outgoing, "dst", split_axis=0, concat_axis=0, tiled=True)
    attn_out = jnp.sum(incoming.astype(jnp.float32), axis=0)
    return attn_out, decode_pool[:, None]


def solution(mesh):
    return jax.shard_map(
        shards,
        mesh=mesh,
        in_specs=(
            P(),
            P(("src", "dst"), None),
            P("dst", "src"),
            P("src", "dst", None, None),
            P(),
            P(),
            P(),
            P(),
        ),
        out_specs=(P(None, "src"), P("src", "dst", None, None)),
        check_vma=False,
    )
```

```python
import functools

import jax
import jax.numpy as jnp
import numpy as np
from jax import lax
from jax.experimental import pallas as pl
from jax.experimental.pallas import tpu as pltpu
from jax.sharding import PartitionSpec as P


QH = 128
KVH = 8
GRP = QH // KVH


NEG_FILL = -1e30
ROPE_BASE = 500000.0

SMEM = pl.BlockSpec(memory_space=pltpu.SMEM)
VMEM = pl.BlockSpec(memory_space=pltpu.VMEM)
ANY = pl.BlockSpec(memory_space=pl.ANY)


def near(array):
    return pltpu.with_memory_space_constraint(array, pltpu.HBM)


def frequencies(head_dim):
    half = np.arange(head_dim // 2, dtype=np.float64)
    frequency = ROPE_BASE ** (-2.0 * half / head_dim)
    return np.concatenate([frequency, frequency]).astype(np.float32)


def pack_body(handoff_in, pool_in, *rest):
    packed, (handoff, count, pool, handoff_sem, pool_sem, page_sem) = rest[:-6], rest[-6:]
    owners = len(packed) + 1
    slots = pool.shape[0]
    group = lax.axis_index("dst") // KVH
    me = lax.axis_index("src")
    first = pltpu.make_async_copy(handoff_in, handoff, handoff_sem)
    whole = pltpu.make_async_copy(pool_in, pool, pool_sem)
    first.start()
    whole.start()
    for offset in range(owners):
        count[offset] = 0
    first.wait()
    whole.wait()

    def send(slot, carry):
        offset = handoff[group, me * slots + slot] ^ me
        place = count[offset]
        count[offset] = place + 1
        for other in range(1, owners):

            @pl.when(offset == other)
            def _(other=other):
                pltpu.make_async_copy(pool.at[slot], packed[other - 1].at[place], page_sem).start()

        return carry

    lax.fori_loop(0, slots, send, 0)

    def settle(index, carry):
        pltpu.make_async_copy(pool.at[0], packed[0].at[0], page_sem).wait()
        return carry

    lax.fori_loop(0, slots - count[0], settle, 0)


def pack(handoff, pool, owners):
    slots = pool.shape[0]
    one = jax.ShapeDtypeStruct((slots // owners + 1,) + pool.shape[1:], pool.dtype)
    return pl.pallas_call(
        pack_body,
        out_shape=[one] * (owners - 1),
        in_specs=[ANY, ANY],
        out_specs=[ANY] * (owners - 1),
        scratch_shapes=[
            pltpu.SMEM(handoff.shape, jnp.int32),
            pltpu.SMEM((owners,), jnp.int32),
            pltpu.VMEM(pool.shape, pool.dtype),
            pltpu.SemaphoreType.DMA,
            pltpu.SemaphoreType.DMA,
            pltpu.SemaphoreType.DMA,
        ],
        compiler_params=pltpu.CompilerParams(vmem_limit_bytes=4 * 1024 * 1024),
        cost_estimate=pl.CostEstimate(flops=10**10, bytes_accessed=2**25, transcendentals=0),
        name="pack",
    )(near(handoff), near(pool))


def project_body(tokens, weight, _after, out, shares, sem):
    groups, heads, rows, head_dim = out.shape
    parts = GRP + 2
    reqs = rows // parts
    depth = weight.shape[0]
    if tokens.shape[1] != depth:
        block = lax.axis_index("src") * lax.axis_size("dst") + lax.axis_index("dst")
        values = tokens[:, pl.ds(pl.multiple_of(block * depth, depth), depth)]
    else:
        values = tokens[...]
    width = parts * head_dim
    for h in range(heads):
        result = jnp.dot(
            values, weight[:, h * width : (h + 1) * width], preferred_element_type=jnp.float32
        )
        for g in range(groups):
            for part in range(parts):
                shares[g, h, part * reqs : (part + 1) * reqs, :] = result[
                    g * reqs : (g + 1) * reqs, part * head_dim : (part + 1) * head_dim
                ]
            pltpu.make_async_copy(shares.at[g, h], out.at[g, h], sem).start()
    pltpu.make_async_copy(shares, out, sem).wait()


def project(tokens, weight, groups, after):
    reqs = tokens.shape[0] // groups
    parts = GRP + 2
    head_dim = weight.shape[1] // (KVH * parts)
    share = jax.ShapeDtypeStruct((groups, KVH, parts * reqs, head_dim), jnp.float32)
    return pl.pallas_call(
        project_body,
        in_specs=[VMEM, VMEM, ANY],
        out_specs=ANY,
        out_shape=share,
        scratch_shapes=[pltpu.VMEM(share.shape, share.dtype), pltpu.SemaphoreType.DMA],
        compiler_params=pltpu.CompilerParams(vmem_limit_bytes=8 * 1024 * 1024),
        name="project",
    )(tokens, weight, after)


def plan_body(
    page_len, slots, handoff, table, lengths, selected, frequency, live, cosine, sine, source, limit
):
    reqs, head_dim = cosine.shape
    me = lax.axis_index("src")
    group = lax.axis_index("dst") // KVH
    head = lax.axis_index("dst") % KVH

    def clear(index, carry):
        limit[index] = 0
        return carry

    lax.fori_loop(0, reqs * slots, clear, 0, unroll=16)
    for r in range(reqs):
        length = lengths[group * reqs + r]

        def mark(entry, carry, r=r, length=length):
            page = selected[group * reqs + r, head, entry]
            slot = table[group * reqs + r, page]
            local = slot - me * slots
            mine = (local >= 0) & (local < slots)
            place = jnp.where(mine, r * slots + local, reqs * slots)
            limit[place] = length - page * page_len
            return carry

        lax.fori_loop(0, selected.shape[2], mark, 0, unroll=8)

    lane = lax.broadcasted_iota(jnp.int32, (1, 128), 1)
    per = 128 // page_len
    for r in range(reqs):
        for chunk in range(slots // per):
            bound = jnp.full((1, 128), limit[r * slots + chunk * per], jnp.int32)
            for k in range(1, per):
                bound = jnp.where(lane >= k * page_len, limit[r * slots + chunk * per + k], bound)
            live[r : r + 1, chunk * 128 : (chunk + 1) * 128] = jnp.where(
                lane % page_len < bound, 1.0, 0.0
            )

    row = lax.broadcasted_iota(jnp.int32, (reqs, head_dim), 0)
    place = lax.broadcasted_iota(jnp.int32, (reqs, head_dim), 1)
    position = jnp.zeros((reqs, head_dim), jnp.float32)
    for r in range(reqs):
        position = jnp.where(row == r, lengths[group * reqs + r].astype(jnp.float32), position)
    angle = frequency[...] * position
    cosine[...] = jnp.cos(angle)
    turn = jnp.sin(angle)
    sine[...] = jnp.where(place < head_dim // 2, -turn, turn)

    owners = handoff.shape[1] // slots

    def owner_pages(owner, filled):
        own = owner == me
        source[owners + (owner ^ me)] = filled

        def look(slot, taken):
            hit = handoff[group, owner * slots + slot] == me
            source[2 * owners + jnp.where(hit & own, taken, slots)] = slot
            return taken + hit.astype(jnp.int32)

        taken = lax.fori_loop(0, slots, look, 0, unroll=8)
        source[owner ^ me] = taken
        return filled + taken

    lax.fori_loop(0, owners, owner_pages, 0)


def plan(handoff, table, lengths, selected, head_dim, reqs, slots, page_len):
    owners = handoff.shape[1] // slots
    frequency = jnp.asarray(frequencies(head_dim))[None]
    return pl.pallas_call(
        functools.partial(plan_body, page_len, slots),
        in_specs=[SMEM] * 4 + [VMEM],
        out_specs=[VMEM] * 3 + [SMEM],
        out_shape=[
            jax.ShapeDtypeStruct((reqs, slots * page_len), jnp.float32),
            jax.ShapeDtypeStruct((reqs, head_dim), jnp.float32),
            jax.ShapeDtypeStruct((reqs, head_dim), jnp.float32),
            jax.ShapeDtypeStruct((2 * owners + slots + 1,), jnp.int32),
        ],
        scratch_shapes=[pltpu.SMEM((reqs * slots + 1,), jnp.int32)],
        compiler_params=pltpu.CompilerParams(vmem_limit_bytes=2 * 1024 * 1024),
        name="plan",
    )(near(handoff), near(table), near(lengths), near(selected), near(frequency))


def attend_body(parts, pool, live, cosine, sine, out):
    total = functools.reduce(jnp.add, [parts[i] for i in range(parts.shape[0])])
    head_dim = total.shape[1]
    reqs = live.shape[0]
    rows = GRP * reqs

    def per_row(values, count):
        row = lax.broadcasted_iota(jnp.int32, (count, 1), 0) % reqs
        wide = jnp.broadcast_to(values[0:1], (count, values.shape[1]))
        for r in range(1, reqs):
            wide = jnp.where(row == r, values[r : r + 1], wide)
        return wide

    turned = total[: rows + reqs]
    turned = turned * per_row(cosine[...], rows + reqs) + pltpu.roll(
        turned, head_dim // 2, 1
    ) * per_row(sine[...], rows + reqs)
    queries = (turned[:rows] * head_dim ** (-0.5)).astype(jnp.bfloat16)
    key_new = per_row(turned[rows:], rows)
    value_new = per_row(total[rows + reqs :], rows)

    pages = pool[...].reshape(-1, 2 * head_dim)
    scores = lax.dot_general(
        queries, pages[:, :head_dim], (((1,), (1,)), ((), ())),
        preferred_element_type=jnp.float32,
    )
    mask = per_row(live[...], rows) > 0.5
    own = jnp.sum(queries.astype(jnp.float32) * key_new, axis=1, keepdims=True)
    first = lax.axis_index("src") == 0
    own = jnp.where(first, own, NEG_FILL)
    top = jnp.maximum(jnp.max(jnp.where(mask, scores, NEG_FILL), axis=1, keepdims=True), own)
    weight = jnp.where(mask, jnp.exp(scores - top), 0.0)
    own_weight = jnp.where(first, jnp.exp(own - top), 0.0)
    total_weight = jnp.sum(weight, axis=1, keepdims=True) + own_weight
    weighted = (
        jnp.dot(
            weight.astype(jnp.bfloat16), pages[:, head_dim:], preferred_element_type=jnp.float32
        )
        + own_weight * value_new
    )
    out[:, :head_dim] = weighted
    lane = lax.broadcasted_iota(jnp.int32, (rows, head_dim), 1)
    out[:, head_dim:] = jnp.where(lane < head_dim // 2, top, total_weight)


def attend(parts, pool, live, cosine, sine):
    reqs = live.shape[0]
    return pl.pallas_call(
        attend_body,
        out_shape=jax.ShapeDtypeStruct((GRP * reqs, pool.shape[2]), jnp.float32),
        in_specs=[VMEM] * 5,
        out_specs=VMEM,
        compiler_params=pltpu.CompilerParams(vmem_limit_bytes=16 * 1024 * 1024),
        cost_estimate=pl.CostEstimate(flops=10**12, bytes_accessed=2**26, transcendentals=0),
        name="attend",
    )(parts, pool, live, cosine, sine)


def merge(parts):
    head_dim = parts.shape[-1] // 2
    half = head_dim + head_dim // 2
    tops = [parts[s, :, head_dim : head_dim + 1] for s in range(parts.shape[0])]
    overall = functools.reduce(jnp.maximum, tops)
    numerator = denominator = 0.0
    for s, top in enumerate(tops):
        factor = jnp.exp(top - overall)
        numerator = numerator + parts[s, :, :head_dim] * factor
        denominator = denominator + parts[s, :, half : half + 1] * factor
    return numerator / denominator


def output_body(merged, source_in, heads, weight, kept_in, *rest):
    owners = (len(rest) - 4) // 2
    pages_in, (out, pool, tokens, source, kept), rest = (
        rest[: owners - 1], rest[owners - 1 : owners + 4], rest[owners + 4 :],
    )
    pages, (bulk_sem, page_sem) = rest[: owners - 1], rest[owners - 1 :]
    bulk = [
        pltpu.make_async_copy(x, y, bulk_sem.at[i])
        for i, (x, y) in enumerate(
            [(source_in, source), (kept_in, kept), *zip(pages_in, pages, strict=True)]
        )
    ]
    for copy in bulk:
        copy.start()

    if merged:
        reqs = tokens.shape[0]
        attended = merge(heads)
        head_dim = attended.shape[1]
        for c in range(GRP):
            tokens[:, c * head_dim : (c + 1) * head_dim] = attended[c * reqs : (c + 1) * reqs]
        values = tokens[...].astype(jnp.bfloat16)
    else:
        values = heads[...]

    def columns(start, tile):
        result = jnp.dot(
            values, weight[:, start : start + tile], preferred_element_type=jnp.float32
        ).astype(out.dtype)
        for copy in range(out.shape[0]):
            out[copy, :, start : start + tile] = result

    width = weight.shape[1]
    tile = width // 8 if width % 1024 == 0 else width
    starts = range(0, width, tile)
    for start in starts[: len(starts) // 2]:
        columns(start, tile)

    for copy in bulk:
        copy.wait()

    def keep(index, carry):
        slot = source[2 * owners + index]
        pltpu.make_async_copy(kept.at[slot], pool.at[source[owners] + index], page_sem).start()
        return carry

    lax.fori_loop(0, source[0], keep, 0)
    for other in range(1, owners):

        def place(index, carry, other=other):
            target = pool.at[source[owners + other] + index]
            pltpu.make_async_copy(pages[other - 1].at[index], target, page_sem).start()
            return carry

        lax.fori_loop(0, source[other], place, 0)

    for start in starts[len(starts) // 2 :]:
        columns(start, tile)
    pltpu.make_async_copy(kept, pool, page_sem).wait()


def output(source, heads, weight, kept, pages, reqs, copies, merged):
    depth, width = weight.shape
    return pl.pallas_call(
        functools.partial(output_body, merged),
        in_specs=[ANY, VMEM, VMEM, ANY] + [ANY] * len(pages),
        out_specs=[VMEM, ANY],
        out_shape=[
            jax.ShapeDtypeStruct((copies, reqs, width), jnp.bfloat16),
            jax.ShapeDtypeStruct(kept.shape, kept.dtype),
        ],
        scratch_shapes=[
            pltpu.VMEM((reqs, depth), jnp.float32),
            pltpu.SMEM(source.shape, jnp.int32),
            pltpu.VMEM(kept.shape, kept.dtype),
            *[pltpu.VMEM(page.shape, page.dtype) for page in pages],
            pltpu.SemaphoreType.DMA((len(pages) + 2,)),
            pltpu.SemaphoreType.DMA,
        ],
        compiler_params=pltpu.CompilerParams(vmem_limit_bytes=12 * 1024 * 1024),
        name="output",
    )(source, heads, weight, kept, *pages)


def shards(normed, qkv_weight, out_weight, prefill_pool, page_table, lengths, selected, handoff):
    owners = lax.axis_size("src")
    decoders = lax.axis_size("dst")
    decoder_id = lax.axis_index("dst")
    groups = decoders // KVH
    reqs = normed.shape[0]
    req_group = reqs // groups
    pool = prefill_pool.reshape(prefill_pool.shape[0], *prefill_pool.shape[2:])
    rows = qkv_weight.shape[0]
    tokens = normed
    if rows % 128:
        row_block = lax.axis_index("src") * decoders + decoder_id
        tokens = lax.dynamic_slice_in_dim(normed, row_block * rows, rows, 1)
    packed = pack(handoff, pool, owners)
    arrived = []
    for k, pages in enumerate(packed):
        arrived.append(lax.ppermute(pages, "src", [(i, i ^ (k + 1)) for i in range(owners)]))
    partial = project(tokens, qkv_weight, groups, packed[0])
    live, cosine, sine, source = plan(
        handoff, page_table, lengths, selected, pool.shape[2] // 2, req_group, pool.shape[0],
        pool.shape[1],
    )
    partial = partial.reshape((decoders,) + partial.shape[2:])
    shares = lax.all_to_all(partial, "dst", split_axis=0, concat_axis=0, tiled=True)
    projected = lax.all_gather(jnp.sum(shares, axis=0), "src")
    mine = attend(projected, pool, live, cosine, sine)
    heads = lax.all_gather(mine, "src")
    merged = groups == 1
    if not merged:
        attended = merge(heads).astype(jnp.bfloat16)
        head_dim = attended.shape[1]
        flat = attended.reshape(GRP, req_group, head_dim).transpose(1, 0, 2)
        every = lax.all_gather(flat.reshape(req_group, -1), "dst", axis=0, tiled=True)
        every = every.reshape(groups, KVH, req_group, -1)
        block = lax.dynamic_index_in_dim(every, decoder_id // groups, 1, keepdims=False)
        depth = out_weight.shape[0]
        heads = lax.dynamic_slice_in_dim(
            block.reshape(reqs, -1), (decoder_id % groups) * depth, depth, 1
        )
    outgoing, decode_pool = output(
        source, heads, out_weight, pool, arrived, reqs, decoders, merged
    )
    incoming = lax.all_to_all(outgoing, "dst", split_axis=0, concat_axis=0, tiled=True)
    attn_out = jnp.sum(incoming.astype(jnp.float32), axis=0)
    return attn_out, decode_pool[:, None]


def solution(mesh):
    return jax.shard_map(
        shards,
        mesh=mesh,
        in_specs=(
            P(),
            P(("src", "dst"), None),
            P("dst", "src"),
            P("src", "dst", None, None),
            P(),
            P(),
            P(),
            P(),
        ),
        out_specs=(P(None, "src"), P("src", "dst", None, None)),
        check_vma=False,
    )
```

```python
import functools

import jax
import jax.numpy as jnp
import numpy as np
from jax import lax
from jax.experimental import pallas as pl
from jax.experimental.pallas import tpu as pltpu
from jax.sharding import PartitionSpec as P


QH = 128
KVH = 8
GRP = QH // KVH


NEG_FILL = -1e30
ROPE_BASE = 500000.0

SMEM = pl.BlockSpec(memory_space=pltpu.SMEM)
VMEM = pl.BlockSpec(memory_space=pltpu.VMEM)
ANY = pl.BlockSpec(memory_space=pl.ANY)


def near(array):
    return pltpu.with_memory_space_constraint(array, pltpu.HBM)


def frequencies(head_dim):
    half = np.arange(head_dim // 2, dtype=np.float64)
    frequency = ROPE_BASE ** (-2.0 * half / head_dim)
    return np.concatenate([frequency, frequency]).astype(np.float32)


def prepare_body(
    reqs, handoff_in, table_in, lengths_in, selected_in, frequency_in, pool_in, *rest
):
    slots, page_len, width = pool_in.shape
    head_dim = width // 2
    owners = handoff_in.shape[1] // slots
    packed, rest = rest[: owners - 1], rest[owners - 1 :]
    live_out, turn_out, source_out, *rest = rest
    handoff, table, lengths, selected, limit, count, source, *rest = rest
    frequency, pool, live, turns, small_sem, pool_sem, page_sem, fact_sem = rest
    me = lax.axis_index("src")
    group = lax.axis_index("dst") // KVH
    head = lax.axis_index("dst") % KVH

    moves = [
        (handoff_in, handoff), (table_in, table), (lengths_in, lengths), (selected_in, selected),
        (frequency_in, frequency),
    ]
    small = [pltpu.make_async_copy(x, y, small_sem.at[i]) for i, (x, y) in enumerate(moves)]
    pool_copy = pltpu.make_async_copy(pool_in, pool, pool_sem)
    for copy in (*small, pool_copy):
        copy.start()

    for offset in range(owners):
        count[offset] = 0
    small[0].wait()
    pool_copy.wait()

    def send(slot, carry):
        offset = handoff[group, me * slots + slot] ^ me
        place = count[offset]
        count[offset] = place + 1
        for other in range(1, owners):

            @pl.when(offset == other)
            def _(other=other):
                pltpu.make_async_copy(pool.at[slot], packed[other - 1].at[place], page_sem).start()

        return carry

    lax.fori_loop(0, slots, send, 0)
    for copy in small[1:]:
        copy.wait()

    def clear(index, carry):
        limit[index] = 0
        return carry

    lax.fori_loop(0, reqs * slots, clear, 0, unroll=16)
    for r in range(reqs):
        length = lengths[group * reqs + r]

        def mark(entry, carry, r=r, length=length):
            page = selected[group * reqs + r, head, entry]
            local = table[group * reqs + r, page] - me * slots
            mine = (local >= 0) & (local < slots)
            limit[jnp.where(mine, r * slots + local, reqs * slots)] = length - page * page_len
            return carry

        lax.fori_loop(0, selected.shape[2], mark, 0, unroll=8)

    lane = lax.broadcasted_iota(jnp.int32, (1, 128), 1)
    per = 128 // page_len
    for r in range(reqs):
        for chunk in range(slots // per):
            bound = jnp.full((1, 128), limit[r * slots + chunk * per], jnp.int32)
            for k in range(1, per):
                bound = jnp.where(lane >= k * page_len, limit[r * slots + chunk * per + k], bound)
            live[r : r + 1, chunk * 128 : (chunk + 1) * 128] = jnp.where(
                lane % page_len < bound, 1.0, 0.0
            )

    row = lax.broadcasted_iota(jnp.int32, (reqs, head_dim), 0)
    place = lax.broadcasted_iota(jnp.int32, (reqs, head_dim), 1)
    position = jnp.zeros((reqs, head_dim), jnp.float32)
    for r in range(reqs):
        position = jnp.where(row == r, lengths[group * reqs + r].astype(jnp.float32), position)
    angle = frequency[...] * position
    turns[0] = jnp.cos(angle)
    sine = jnp.sin(angle)
    turns[1] = jnp.where(place < head_dim // 2, -sine, sine)

    def owner_pages(owner, filled):
        own = owner == me
        source[owners + (owner ^ me)] = filled

        def look(slot, taken):
            hit = handoff[group, owner * slots + slot] == me
            source[2 * owners + jnp.where(hit & own, taken, slots)] = slot
            return taken + hit.astype(jnp.int32)

        taken = lax.fori_loop(0, slots, look, 0, unroll=8)
        source[owner ^ me] = taken
        return filled + taken

    lax.fori_loop(0, owners, owner_pages, 0)
    facts = [
        pltpu.make_async_copy(x, y, fact_sem.at[i])
        for i, (x, y) in enumerate([(live, live_out), (turns, turn_out), (source, source_out)])
    ]
    for copy in facts:
        copy.start()

    for copy in facts:
        copy.wait()

    def settle(index, carry):
        pltpu.make_async_copy(pool.at[0], packed[0].at[0], page_sem).wait()
        return carry

    lax.fori_loop(0, slots - count[0], settle, 0)


def prepare(handoff, table, lengths, selected, pool, reqs, owners):
    slots, page_len, width = pool.shape
    head_dim = width // 2
    frequency = jnp.asarray(frequencies(head_dim))[None]
    page = jax.ShapeDtypeStruct((slots // owners + 1, page_len, width), pool.dtype)
    live = jax.ShapeDtypeStruct((reqs, slots * page_len), jnp.float32)
    turns = jax.ShapeDtypeStruct((2, reqs, head_dim), jnp.float32)
    source = jax.ShapeDtypeStruct((2 * owners + slots + 1,), jnp.int32)
    integers = [handoff, table, lengths, selected]
    *packed, live, turns, source = pl.pallas_call(
        functools.partial(prepare_body, reqs),
        in_specs=[ANY] * 6,
        out_specs=[ANY] * (owners + 2),
        out_shape=[page] * (owners - 1) + [live, turns, source],
        scratch_shapes=[pltpu.SMEM(a.shape, jnp.int32) for a in integers]
        + [
            pltpu.SMEM((reqs * slots + 1,), jnp.int32),
            pltpu.SMEM((owners,), jnp.int32),
            pltpu.SMEM(source.shape, jnp.int32),
            pltpu.VMEM(frequency.shape, jnp.float32),
            pltpu.VMEM(pool.shape, pool.dtype),
            pltpu.VMEM(live.shape, live.dtype),
            pltpu.VMEM(turns.shape, turns.dtype),
            pltpu.SemaphoreType.DMA((5,)),
            pltpu.SemaphoreType.DMA,
            pltpu.SemaphoreType.DMA,
            pltpu.SemaphoreType.DMA((3,)),
        ],
        compiler_params=pltpu.CompilerParams(vmem_limit_bytes=4 * 1024 * 1024),
        cost_estimate=pl.CostEstimate(flops=10**10, bytes_accessed=2**25, transcendentals=0),
        name="prepare",
    )(*map(near, integers), near(frequency), near(pool))
    return packed, live, turns, source


def project_body(tokens, weight, _after, out):
    groups, heads, rows, head_dim = out.shape
    parts = GRP + 2
    reqs = rows // parts
    depth = weight.shape[0]
    if tokens.shape[1] != depth:
        block = lax.axis_index("src") * lax.axis_size("dst") + lax.axis_index("dst")
        values = tokens[:, pl.ds(pl.multiple_of(block * depth, depth), depth)]
    else:
        values = tokens[...]
    width = parts * head_dim
    for h in range(heads):
        result = jnp.dot(
            values, weight[:, h * width : (h + 1) * width], preferred_element_type=jnp.float32
        )
        for g in range(groups):
            for part in range(parts):
                out[g, h, part * reqs : (part + 1) * reqs, :] = result[
                    g * reqs : (g + 1) * reqs, part * head_dim : (part + 1) * head_dim
                ]


def project(tokens, weight, groups, after):
    reqs = tokens.shape[0] // groups
    parts = GRP + 2
    head_dim = weight.shape[1] // (KVH * parts)
    return pl.pallas_call(
        project_body,
        in_specs=[VMEM, VMEM, ANY],
        out_specs=VMEM,
        out_shape=jax.ShapeDtypeStruct((groups, KVH, parts * reqs, head_dim), jnp.float32),
        compiler_params=pltpu.CompilerParams(vmem_limit_bytes=8 * 1024 * 1024),
        name="project",
    )(tokens, weight, after)


def attend_body(parts, pool, live, turns, out):
    total = functools.reduce(jnp.add, [parts[i] for i in range(parts.shape[0])])
    head_dim = total.shape[1]
    reqs = live.shape[0]
    rows = GRP * reqs

    def per_row(values, count):
        row = lax.broadcasted_iota(jnp.int32, (count, 1), 0) % reqs
        wide = jnp.broadcast_to(values[0:1], (count, values.shape[1]))
        for r in range(1, reqs):
            wide = jnp.where(row == r, values[r : r + 1], wide)
        return wide

    turned = total[: rows + reqs]
    turned = turned * per_row(turns[0], rows + reqs) + pltpu.roll(
        turned, head_dim // 2, 1
    ) * per_row(turns[1], rows + reqs)
    queries = (turned[:rows] * head_dim ** (-0.5)).astype(jnp.bfloat16)
    key_new = per_row(turned[rows:], rows)
    value_new = per_row(total[rows + reqs :], rows)

    pages = pool[...].reshape(-1, 2 * head_dim)
    scores = lax.dot_general(
        queries, pages[:, :head_dim], (((1,), (1,)), ((), ())),
        preferred_element_type=jnp.float32,
    )
    mask = per_row(live[...], rows) > 0.5
    own = jnp.sum(queries.astype(jnp.float32) * key_new, axis=1, keepdims=True)
    first = lax.axis_index("src") == 0
    own = jnp.where(first, own, NEG_FILL)
    top = jnp.maximum(jnp.max(jnp.where(mask, scores, NEG_FILL), axis=1, keepdims=True), own)
    weight = jnp.where(mask, jnp.exp(scores - top), 0.0)
    own_weight = jnp.where(first, jnp.exp(own - top), 0.0)
    total_weight = jnp.sum(weight, axis=1, keepdims=True) + own_weight
    weighted = (
        jnp.dot(
            weight.astype(jnp.bfloat16), pages[:, head_dim:], preferred_element_type=jnp.float32
        )
        + own_weight * value_new
    )
    out[:, :head_dim] = weighted
    lane = lax.broadcasted_iota(jnp.int32, (rows, head_dim), 1)
    out[:, head_dim:] = jnp.where(lane < head_dim // 2, top, total_weight)


def attend(parts, pool, live, turns):
    reqs = live.shape[0]
    return pl.pallas_call(
        attend_body,
        out_shape=jax.ShapeDtypeStruct((GRP * reqs, pool.shape[2]), jnp.float32),
        in_specs=[VMEM] * 4,
        out_specs=VMEM,
        compiler_params=pltpu.CompilerParams(vmem_limit_bytes=16 * 1024 * 1024),
        cost_estimate=pl.CostEstimate(flops=10**12, bytes_accessed=2**26, transcendentals=0),
        name="attend",
    )(parts, pool, live, turns)


def merge(parts):
    head_dim = parts.shape[-1] // 2
    half = head_dim + head_dim // 2
    tops = [parts[s, :, head_dim : head_dim + 1] for s in range(parts.shape[0])]
    overall = functools.reduce(jnp.maximum, tops)
    numerator = denominator = 0.0
    for s, top in enumerate(tops):
        factor = jnp.exp(top - overall)
        numerator = numerator + parts[s, :, :head_dim] * factor
        denominator = denominator + parts[s, :, half : half + 1] * factor
    return numerator / denominator


def output_body(merged, source_in, heads, weight, kept_in, *rest):
    owners = (len(rest) - 4) // 2
    pages_in, (out, pool, tokens, source, kept), rest = (
        rest[: owners - 1], rest[owners - 1 : owners + 4], rest[owners + 4 :],
    )
    pages, (bulk_sem, page_sem) = rest[: owners - 1], rest[owners - 1 :]
    bulk = [
        pltpu.make_async_copy(x, y, bulk_sem.at[i])
        for i, (x, y) in enumerate(
            [(source_in, source), (kept_in, kept), *zip(pages_in, pages, strict=True)]
        )
    ]
    for copy in bulk:
        copy.start()

    if merged:
        reqs = tokens.shape[0]
        attended = merge(heads)
        head_dim = attended.shape[1]
        for c in range(GRP):
            tokens[:, c * head_dim : (c + 1) * head_dim] = attended[c * reqs : (c + 1) * reqs]
        values = tokens[...].astype(jnp.bfloat16)
    else:
        values = heads[...]

    def columns(start, tile):
        result = jnp.dot(
            values, weight[:, start : start + tile], preferred_element_type=jnp.float32
        ).astype(out.dtype)
        for copy in range(out.shape[0]):
            out[copy, :, start : start + tile] = result

    width = weight.shape[1]
    tile = width // 8 if width % 1024 == 0 else width
    starts = range(0, width, tile)
    for start in starts[: len(starts) // 2]:
        columns(start, tile)

    for copy in bulk:
        copy.wait()

    def keep(index, carry):
        slot = source[2 * owners + index]
        pltpu.make_async_copy(kept.at[slot], pool.at[source[owners] + index], page_sem).start()
        return carry

    lax.fori_loop(0, source[0], keep, 0)
    for other in range(1, owners):

        def place(index, carry, other=other):
            target = pool.at[source[owners + other] + index]
            pltpu.make_async_copy(pages[other - 1].at[index], target, page_sem).start()
            return carry

        lax.fori_loop(0, source[other], place, 0)

    for start in starts[len(starts) // 2 :]:
        columns(start, tile)
    pltpu.make_async_copy(kept, pool, page_sem).wait()


def output(source, heads, weight, kept, pages, reqs, copies, merged):
    depth, width = weight.shape
    return pl.pallas_call(
        functools.partial(output_body, merged),
        in_specs=[ANY, VMEM, VMEM, ANY] + [ANY] * len(pages),
        out_specs=[VMEM, ANY],
        out_shape=[
            jax.ShapeDtypeStruct((copies, reqs, width), jnp.bfloat16),
            jax.ShapeDtypeStruct(kept.shape, kept.dtype),
        ],
        scratch_shapes=[
            pltpu.VMEM((reqs, depth), jnp.float32),
            pltpu.SMEM(source.shape, jnp.int32),
            pltpu.VMEM(kept.shape, kept.dtype),
            *[pltpu.VMEM(page.shape, page.dtype) for page in pages],
            pltpu.SemaphoreType.DMA((len(pages) + 2,)),
            pltpu.SemaphoreType.DMA,
        ],
        compiler_params=pltpu.CompilerParams(vmem_limit_bytes=12 * 1024 * 1024),
        name="output",
    )(source, heads, weight, kept, *pages)


def shards(normed, qkv_weight, out_weight, prefill_pool, page_table, lengths, selected, handoff):
    owners = lax.axis_size("src")
    decoders = lax.axis_size("dst")
    decoder_id = lax.axis_index("dst")
    groups = decoders // KVH
    reqs = normed.shape[0]
    req_group = reqs // groups
    pool = prefill_pool.reshape(prefill_pool.shape[0], *prefill_pool.shape[2:])
    rows = qkv_weight.shape[0]
    tokens = normed
    if rows % 128:
        row_block = lax.axis_index("src") * decoders + decoder_id
        tokens = lax.dynamic_slice_in_dim(normed, row_block * rows, rows, 1)
    packed, live, turns, source = prepare(
        handoff, page_table, lengths, selected, pool, req_group, owners
    )
    arrived = []
    for k, pages in enumerate(packed):
        arrived.append(lax.ppermute(pages, "src", [(i, i ^ (k + 1)) for i in range(owners)]))
    partial = project(tokens, qkv_weight, groups, packed[0])
    partial = partial.reshape((decoders,) + partial.shape[2:])
    shares = lax.all_to_all(partial, "dst", split_axis=0, concat_axis=0, tiled=True)
    projected = lax.all_gather(jnp.sum(shares, axis=0), "src")
    mine = attend(projected, pool, live, turns)
    heads = lax.all_gather(mine, "src")
    merged = groups == 1
    if not merged:
        attended = merge(heads).astype(jnp.bfloat16)
        head_dim = attended.shape[1]
        flat = attended.reshape(GRP, req_group, head_dim).transpose(1, 0, 2)
        every = lax.all_gather(flat.reshape(req_group, -1), "dst", axis=0, tiled=True)
        every = every.reshape(groups, KVH, req_group, -1)
        block = lax.dynamic_index_in_dim(every, decoder_id // groups, 1, keepdims=False)
        depth = out_weight.shape[0]
        heads = lax.dynamic_slice_in_dim(
            block.reshape(reqs, -1), (decoder_id % groups) * depth, depth, 1
        )
    outgoing, decode_pool = output(
        source, heads, out_weight, pool, arrived, reqs, decoders, merged
    )
    incoming = lax.all_to_all(outgoing, "dst", split_axis=0, concat_axis=0, tiled=True)
    attn_out = jnp.sum(incoming.astype(jnp.float32), axis=0)
    return attn_out, decode_pool[:, None]


def solution(mesh):
    return jax.shard_map(
        shards,
        mesh=mesh,
        in_specs=(
            P(),
            P(("src", "dst"), None),
            P("dst", "src"),
            P("src", "dst", None, None),
            P(),
            P(),
            P(),
            P(),
        ),
        out_specs=(P(None, "src"), P("src", "dst", None, None)),
        check_vma=False,
    )
```

```python
import functools

import jax
import jax.numpy as jnp
import numpy as np
from jax import lax
from jax.experimental import pallas as pl
from jax.experimental.pallas import tpu as pltpu
from jax.sharding import PartitionSpec as P


QH = 128
KVH = 8
GRP = QH // KVH


NEG_FILL = -1e30
ROPE_BASE = 500000.0

SMEM = pl.BlockSpec(memory_space=pltpu.SMEM)
VMEM = pl.BlockSpec(memory_space=pltpu.VMEM)
ANY = pl.BlockSpec(memory_space=pl.ANY)


def near(array):
    return pltpu.with_memory_space_constraint(array, pltpu.HBM)


def frequencies(head_dim):
    half = np.arange(head_dim // 2, dtype=np.float64)
    frequency = ROPE_BASE ** (-2.0 * half / head_dim)
    return np.concatenate([frequency, frequency]).astype(np.float32)


def prepare_body(
    reqs, handoff_in, table_in, lengths_in, selected_in, frequency_in, pool_in, *rest
):
    slots, page_len, width = pool_in.shape
    head_dim = width // 2
    owners = handoff_in.shape[1] // slots
    packed, rest = rest[: owners - 1], rest[owners - 1 :]
    live_out, turn_out, source_out, *rest = rest
    handoff, table, lengths, selected, limit, count, source, *rest = rest
    frequency, pool, live, turns, small_sem, pool_sem, page_sem, fact_sem = rest
    me = lax.axis_index("src")
    group = lax.axis_index("dst") // KVH
    head = lax.axis_index("dst") % KVH

    moves = [
        (handoff_in, handoff), (table_in, table), (lengths_in, lengths), (selected_in, selected),
        (frequency_in, frequency),
    ]
    small = [pltpu.make_async_copy(x, y, small_sem.at[i]) for i, (x, y) in enumerate(moves)]
    pool_copy = pltpu.make_async_copy(pool_in, pool, pool_sem)
    for copy in (*small, pool_copy):
        copy.start()

    for offset in range(owners):
        count[offset] = 0
    small[0].wait()
    pool_copy.wait()

    def send(slot, carry):
        offset = handoff[group, me * slots + slot] ^ me
        place = count[offset]
        count[offset] = place + 1
        for other in range(1, owners):

            @pl.when(offset == other)
            def _(other=other):
                pltpu.make_async_copy(pool.at[slot], packed[other - 1].at[place], page_sem).start()

        return carry

    lax.fori_loop(0, slots, send, 0)
    for copy in small[1:]:
        copy.wait()

    def clear(index, carry):
        limit[index] = 0
        return carry

    lax.fori_loop(0, reqs * slots, clear, 0, unroll=16)
    for r in range(reqs):
        length = lengths[group * reqs + r]

        def mark(entry, carry, r=r, length=length):
            page = selected[group * reqs + r, head, entry]
            local = table[group * reqs + r, page] - me * slots
            mine = (local >= 0) & (local < slots)
            limit[jnp.where(mine, r * slots + local, reqs * slots)] = length - page * page_len
            return carry

        lax.fori_loop(0, selected.shape[2], mark, 0, unroll=8)

    lane = lax.broadcasted_iota(jnp.int32, (1, 128), 1)
    per = 128 // page_len
    for r in range(reqs):
        for chunk in range(slots // per):
            bound = jnp.full((1, 128), limit[r * slots + chunk * per], jnp.int32)
            for k in range(1, per):
                bound = jnp.where(lane >= k * page_len, limit[r * slots + chunk * per + k], bound)
            live[r : r + 1, chunk * 128 : (chunk + 1) * 128] = jnp.where(
                lane % page_len < bound, 1.0, 0.0
            )

    row = lax.broadcasted_iota(jnp.int32, (reqs, head_dim), 0)
    place = lax.broadcasted_iota(jnp.int32, (reqs, head_dim), 1)
    position = jnp.zeros((reqs, head_dim), jnp.float32)
    for r in range(reqs):
        position = jnp.where(row == r, lengths[group * reqs + r].astype(jnp.float32), position)
    angle = frequency[...] * position
    turns[0] = jnp.cos(angle)
    sine = jnp.sin(angle)
    turns[1] = jnp.where(place < head_dim // 2, -sine, sine)

    def owner_pages(owner, filled):
        own = owner == me
        source[owners + (owner ^ me)] = filled

        def look(slot, taken):
            hit = handoff[group, owner * slots + slot] == me
            source[2 * owners + jnp.where(hit & own, taken, slots)] = slot
            return taken + hit.astype(jnp.int32)

        taken = lax.fori_loop(0, slots, look, 0, unroll=8)
        source[owner ^ me] = taken
        return filled + taken

    lax.fori_loop(0, owners, owner_pages, 0)
    facts = [
        pltpu.make_async_copy(x, y, fact_sem.at[i])
        for i, (x, y) in enumerate([(live, live_out), (turns, turn_out), (source, source_out)])
    ]
    for copy in facts:
        copy.start()

    for copy in facts:
        copy.wait()

    def settle(index, carry):
        pltpu.make_async_copy(pool.at[0], packed[0].at[0], page_sem).wait()
        return carry

    lax.fori_loop(0, slots - count[0], settle, 0)


def prepare(handoff, table, lengths, selected, pool, reqs, owners):
    slots, page_len, width = pool.shape
    head_dim = width // 2
    frequency = jnp.asarray(frequencies(head_dim))[None]
    page = jax.ShapeDtypeStruct((slots // owners + 1, page_len, width), pool.dtype)
    live = jax.ShapeDtypeStruct((reqs, slots * page_len), jnp.float32)
    turns = jax.ShapeDtypeStruct((2, reqs, head_dim), jnp.float32)
    source = jax.ShapeDtypeStruct((2 * owners + slots + 1,), jnp.int32)
    integers = [handoff, table, lengths, selected]
    *packed, live, turns, source = pl.pallas_call(
        functools.partial(prepare_body, reqs),
        in_specs=[ANY] * 6,
        out_specs=[ANY] * (owners + 2),
        out_shape=[page] * (owners - 1) + [live, turns, source],
        scratch_shapes=[pltpu.SMEM(a.shape, jnp.int32) for a in integers]
        + [
            pltpu.SMEM((reqs * slots + 1,), jnp.int32),
            pltpu.SMEM((owners,), jnp.int32),
            pltpu.SMEM(source.shape, jnp.int32),
            pltpu.VMEM(frequency.shape, jnp.float32),
            pltpu.VMEM(pool.shape, pool.dtype),
            pltpu.VMEM(live.shape, live.dtype),
            pltpu.VMEM(turns.shape, turns.dtype),
            pltpu.SemaphoreType.DMA((5,)),
            pltpu.SemaphoreType.DMA,
            pltpu.SemaphoreType.DMA,
            pltpu.SemaphoreType.DMA((3,)),
        ],
        compiler_params=pltpu.CompilerParams(vmem_limit_bytes=4 * 1024 * 1024),
        cost_estimate=pl.CostEstimate(flops=10**10, bytes_accessed=2**25, transcendentals=0),
        name="prepare",
    )(*map(near, integers), near(frequency), near(pool))
    return packed, live, turns, source


def project_body(tokens, weight, _after, out):
    groups, heads, reqs, width = out.shape
    depth = weight.shape[0]
    if tokens.shape[1] != depth:
        block = lax.axis_index("src") * lax.axis_size("dst") + lax.axis_index("dst")
        values = tokens[:, pl.ds(pl.multiple_of(block * depth, depth), depth)]
    else:
        values = tokens[...]
    for h in range(heads):
        result = jnp.dot(
            values, weight[:, h * width : (h + 1) * width], preferred_element_type=jnp.float32
        )
        for g in range(groups):
            out[g, h] = result[g * reqs : (g + 1) * reqs]


def project(tokens, weight, groups, after):
    reqs, width = tokens.shape[0] // groups, weight.shape[1] // KVH
    return pl.pallas_call(
        project_body,
        in_specs=[VMEM, VMEM, ANY],
        out_specs=VMEM,
        out_shape=jax.ShapeDtypeStruct((groups, KVH, reqs, width), jnp.float32),
        compiler_params=pltpu.CompilerParams(vmem_limit_bytes=8 * 1024 * 1024),
        name="project",
    )(tokens, weight, after)


def attend_body(shares, pool, live, turns, out, split):
    head_dim = split.shape[1]
    reqs = live.shape[0]
    joined = functools.reduce(jnp.add, [shares[i] for i in range(shares.shape[0])])
    for part in range(GRP + 2):
        split[part * reqs : (part + 1) * reqs] = joined[:, part * head_dim : (part + 1) * head_dim]
    total = split[...]
    rows = GRP * reqs

    def per_row(values, count):
        row = lax.broadcasted_iota(jnp.int32, (count, 1), 0) % reqs
        wide = jnp.broadcast_to(values[0:1], (count, values.shape[1]))
        for r in range(1, reqs):
            wide = jnp.where(row == r, values[r : r + 1], wide)
        return wide

    turned = total[: rows + reqs]
    turned = turned * per_row(turns[0], rows + reqs) + pltpu.roll(
        turned, head_dim // 2, 1
    ) * per_row(turns[1], rows + reqs)
    queries = (turned[:rows] * head_dim ** (-0.5)).astype(jnp.bfloat16)
    key_new = per_row(turned[rows:], rows)
    value_new = per_row(total[rows + reqs :], rows)

    pages = pool[...].reshape(-1, 2 * head_dim)
    scores = lax.dot_general(
        queries, pages[:, :head_dim], (((1,), (1,)), ((), ())),
        preferred_element_type=jnp.float32,
    )
    mask = per_row(live[...], rows) > 0.5
    own = jnp.sum(queries.astype(jnp.float32) * key_new, axis=1, keepdims=True)
    first = lax.axis_index("src") == 0
    own = jnp.where(first, own, NEG_FILL)
    top = jnp.maximum(jnp.max(jnp.where(mask, scores, NEG_FILL), axis=1, keepdims=True), own)
    weight = jnp.where(mask, jnp.exp(scores - top), 0.0)
    own_weight = jnp.where(first, jnp.exp(own - top), 0.0)
    total_weight = jnp.sum(weight, axis=1, keepdims=True) + own_weight
    weighted = (
        jnp.dot(
            weight.astype(jnp.bfloat16), pages[:, head_dim:], preferred_element_type=jnp.float32
        )
        + own_weight * value_new
    )
    out[:, :head_dim] = weighted
    lane = lax.broadcasted_iota(jnp.int32, (rows, head_dim), 1)
    out[:, head_dim:] = jnp.where(lane < head_dim // 2, top, total_weight)


def attend(shares, pool, live, turns):
    reqs = live.shape[0]
    return pl.pallas_call(
        attend_body,
        out_shape=jax.ShapeDtypeStruct((GRP * reqs, pool.shape[2]), jnp.float32),
        in_specs=[VMEM] * 4,
        out_specs=VMEM,
        scratch_shapes=[pltpu.VMEM(((GRP + 2) * reqs, pool.shape[2] // 2), jnp.float32)],
        compiler_params=pltpu.CompilerParams(vmem_limit_bytes=16 * 1024 * 1024),
        cost_estimate=pl.CostEstimate(flops=10**12, bytes_accessed=2**26, transcendentals=0),
        name="attend",
    )(shares, pool, live, turns)


def merge(parts):
    head_dim = parts.shape[-1] // 2
    half = head_dim + head_dim // 2
    tops = [parts[s, :, head_dim : head_dim + 1] for s in range(parts.shape[0])]
    overall = functools.reduce(jnp.maximum, tops)
    numerator = denominator = 0.0
    for s, top in enumerate(tops):
        factor = jnp.exp(top - overall)
        numerator = numerator + parts[s, :, :head_dim] * factor
        denominator = denominator + parts[s, :, half : half + 1] * factor
    return numerator / denominator


def output_body(merged, source_in, heads, weight, kept_in, *rest):
    owners = (len(rest) - 4) // 2
    pages_in, (out, pool, tokens, source, kept), rest = (
        rest[: owners - 1], rest[owners - 1 : owners + 4], rest[owners + 4 :],
    )
    pages, (bulk_sem, page_sem) = rest[: owners - 1], rest[owners - 1 :]
    bulk = [
        pltpu.make_async_copy(x, y, bulk_sem.at[i])
        for i, (x, y) in enumerate(
            [(source_in, source), (kept_in, kept), *zip(pages_in, pages, strict=True)]
        )
    ]
    for copy in bulk:
        copy.start()

    if merged:
        reqs = tokens.shape[0]
        attended = merge(heads)
        head_dim = attended.shape[1]
        for c in range(GRP):
            tokens[:, c * head_dim : (c + 1) * head_dim] = attended[c * reqs : (c + 1) * reqs]
        values = tokens[...].astype(jnp.bfloat16)
    else:
        values = heads[...]

    def columns(start, tile):
        result = jnp.dot(
            values, weight[:, start : start + tile], preferred_element_type=jnp.float32
        ).astype(out.dtype)
        for copy in range(out.shape[0]):
            out[copy, :, start : start + tile] = result

    width = weight.shape[1]
    tile = width // 8 if width % 1024 == 0 else width
    starts = range(0, width, tile)
    for start in starts[: len(starts) // 2]:
        columns(start, tile)

    for copy in bulk:
        copy.wait()

    def keep(index, carry):
        slot = source[2 * owners + index]
        pltpu.make_async_copy(kept.at[slot], pool.at[source[owners] + index], page_sem).start()
        return carry

    lax.fori_loop(0, source[0], keep, 0)
    for other in range(1, owners):

        def place(index, carry, other=other):
            target = pool.at[source[owners + other] + index]
            pltpu.make_async_copy(pages[other - 1].at[index], target, page_sem).start()
            return carry

        lax.fori_loop(0, source[other], place, 0)

    for start in starts[len(starts) // 2 :]:
        columns(start, tile)
    pltpu.make_async_copy(kept, pool, page_sem).wait()


def output(source, heads, weight, kept, pages, reqs, copies, merged):
    depth, width = weight.shape
    return pl.pallas_call(
        functools.partial(output_body, merged),
        in_specs=[ANY, VMEM, VMEM, ANY] + [ANY] * len(pages),
        out_specs=[VMEM, ANY],
        out_shape=[
            jax.ShapeDtypeStruct((copies, reqs, width), jnp.bfloat16),
            jax.ShapeDtypeStruct(kept.shape, kept.dtype),
        ],
        scratch_shapes=[
            pltpu.VMEM((reqs, depth), jnp.float32),
            pltpu.SMEM(source.shape, jnp.int32),
            pltpu.VMEM(kept.shape, kept.dtype),
            *[pltpu.VMEM(page.shape, page.dtype) for page in pages],
            pltpu.SemaphoreType.DMA((len(pages) + 2,)),
            pltpu.SemaphoreType.DMA,
        ],
        compiler_params=pltpu.CompilerParams(vmem_limit_bytes=12 * 1024 * 1024),
        name="output",
    )(source, heads, weight, kept, *pages)


def shards(normed, qkv_weight, out_weight, prefill_pool, page_table, lengths, selected, handoff):
    owners = lax.axis_size("src")
    decoders = lax.axis_size("dst")
    decoder_id = lax.axis_index("dst")
    groups = decoders // KVH
    reqs = normed.shape[0]
    req_group = reqs // groups
    pool = prefill_pool.reshape(prefill_pool.shape[0], *prefill_pool.shape[2:])
    rows = qkv_weight.shape[0]
    tokens = normed
    if rows % 128:
        row_block = lax.axis_index("src") * decoders + decoder_id
        tokens = lax.dynamic_slice_in_dim(normed, row_block * rows, rows, 1)
    packed, live, turns, source = prepare(
        handoff, page_table, lengths, selected, pool, req_group, owners
    )
    arrived = []
    for k, pages in enumerate(packed):
        arrived.append(lax.ppermute(pages, "src", [(i, i ^ (k + 1)) for i in range(owners)]))
    partial = project(tokens, qkv_weight, groups, packed[0])
    partial = partial.reshape((decoders,) + partial.shape[2:])
    shares = lax.all_to_all(partial, "dst", split_axis=0, concat_axis=0, tiled=True)
    projected = lax.all_gather(jnp.sum(shares, axis=0), "src")
    mine = attend(projected, pool, live, turns)
    heads = lax.all_gather(mine, "src")
    merged = groups == 1
    if not merged:
        attended = merge(heads).astype(jnp.bfloat16)
        head_dim = attended.shape[1]
        flat = attended.reshape(GRP, req_group, head_dim).transpose(1, 0, 2)
        every = lax.all_gather(flat.reshape(req_group, -1), "dst", axis=0, tiled=True)
        every = every.reshape(groups, KVH, req_group, -1)
        block = lax.dynamic_index_in_dim(every, decoder_id // groups, 1, keepdims=False)
        depth = out_weight.shape[0]
        heads = lax.dynamic_slice_in_dim(
            block.reshape(reqs, -1), (decoder_id % groups) * depth, depth, 1
        )
    outgoing, decode_pool = output(
        source, heads, out_weight, pool, arrived, reqs, decoders, merged
    )
    incoming = lax.all_to_all(outgoing, "dst", split_axis=0, concat_axis=0, tiled=True)
    attn_out = jnp.sum(incoming.astype(jnp.float32), axis=0)
    return attn_out, decode_pool[:, None]


def solution(mesh):
    return jax.shard_map(
        shards,
        mesh=mesh,
        in_specs=(
            P(),
            P(("src", "dst"), None),
            P("dst", "src"),
            P("src", "dst", None, None),
            P(),
            P(),
            P(),
            P(),
        ),
        out_specs=(P(None, "src"), P("src", "dst", None, None)),
        check_vma=False,
    )
```
